32 devices in a mesh: gx: 4 (over y, x), gy: 4 (over z), layer: 2 (over core).
Axes of the slice: x: 2, y: 2, z: 4, core: 2. Of those that a mesh axis runs over, the one named last changes fastest.
Arguments:
- profiles: bfloat16 [2, 4, 65536, 256], P('layer', 'gx', 'gy'), may hold values from 0.049804688 to 2
- time_weight: bfloat16 [256], replicated, may hold values from 0 to 0.029907227
- slot_cell: int32 [2, 4, 65536], P('layer', 'gx', 'gy'), may hold values from 0 to 65535
- inst_count: int32 [2, 4, 4], P('layer', 'gx', 'gy'), may hold values from 1 to 16384, as said below
- metal: float32 [6, 512, 2048], P('layer', 'gx', 'gy'), may hold values from 0.5 to 4
- via_density: float32 [512, 2048], P('gx', 'gy'), may hold values from 0.5 to 4
- pad: float32 [512, 2048], P('gx', 'gy'), may hold values from 0.05 to 0.5
- start_drop: float32 [6, 512, 2048], P('layer', 'gx', 'gy'), may hold values from 0 to 1
Outputs:
- drop: float32 [6, 512, 2048], P('layer', 'gx', 'gy')
- residual: float32 [6, 512, 2048], P('layer', 'gx', 'gy')
The draws below stay inside these ranges and needn't reach their ends.
Inputs may be any that keep to these rules, and one draw needn't show every extreme that they name: The first inst_count slots of a device are live, the rest are padding; and one device is full in every draw. `slot_cell`: row-major cell index within the tile of 128 x 512 cells.
All inputs are finite; a program needn't handle non-finite values.
Results may differ from the reference program's by a relative error of at most 0.0018.
Values sent between devices are 32-bit elements; how exact they have to be, the bound alone decides.
A program may use at most 64 MiB of HBM per device.

```python
import math
import jax
import jax.numpy as jnp

CX = 128
CY = 512
INST_DEV = 16384
TIME = 256
ITERS = 3
GROUPS = 2
TILES_X = 4
TILES_Y = 4
NL = 6
NX = 512
NY = 2048


def draw_inst_count(key, part):
    key_factor, key_group, key_column = jax.random.split(jax.random.fold_in(key, 17), 3)
    tile_rows = jnp.arange(TILES_Y, dtype=jnp.int32)
    base_count = INST_DEV * (TILES_Y - 1 + 5 * tile_rows) // (6 * (TILES_Y - 1))
    factor = jax.random.randint(key_factor, (GROUPS, TILES_X, TILES_Y), 70, 101)
    counts = jnp.maximum(base_count[None, None, :] * factor // 100, 1)
    group_pick = jax.random.randint(key_group, (), 0, GROUPS)
    column_pick = jax.random.randint(key_column, (), 0, TILES_X)
    counts = counts.at[group_pick, column_pick, TILES_Y - 1].set(INST_DEV)
    return counts.astype(jnp.int32)


def with_ends(values, rng, low, top_value):
    longest = values.shape.index(max(values.shape))
    spots = []
    for shift in (0, 1):
        where = [jax.random.randint(jax.random.fold_in(rng, axis), (), 0, length) for axis, length in enumerate(values.shape)]
        where[longest] = (where[longest] + shift) % values.shape[longest]
        spots.append(tuple(where))
    return values.at[spots[0]].set(low).at[spots[1]].set(top_value)


def steps_of(key, shape, cuts, least, largest):
    gain, own = 1.0, jax.random.fold_in(key, 6)
    for axis_at, parts in cuts:
        draws = jnp.exp(jax.random.uniform(jax.random.fold_in(own, axis_at), (parts,), jnp.float32, least / len(cuts), largest / len(cuts)))
        gain = gain * jnp.repeat(draws, shape[axis_at] // parts).reshape([-1 if axis == axis_at else 1 for axis in range(len(shape))])
    return gain


def setup_inputs(seed: int = 0) -> dict:
    streams_of = jax.random.split(jax.random.key(seed), 9)
    return {
        "profiles": jnp.clip(jnp.exp(math.log(2.0) - 3.6927934 * jax.random.uniform(streams_of[0], (GROUPS, TILES_X, TILES_Y * INST_DEV, TIME), jnp.float32) ** steps_of(streams_of[0], (GROUPS, TILES_X, TILES_Y * INST_DEV, TIME), ((0, 2), (1, 4), (2, 4)), -0.2, 0.2)), 0.049804688, 2.0).astype(jnp.bfloat16),
        "time_weight": jnp.clip(jax.random.uniform(streams_of[1], (TIME,), jnp.float32, 0.0, 0.029907227), 0.0, 0.029907227).astype(jnp.bfloat16),
        "slot_cell": with_ends(jax.random.randint(streams_of[2], (GROUPS, TILES_X, TILES_Y * INST_DEV), 0, CX * CY), jax.random.fold_in(streams_of[2], 1), 0, (CX * CY) - 1).astype(jnp.int32),
        "inst_count": draw_inst_count(jax.random.fold_in(streams_of[8], 71), 0),
        "metal": jnp.clip(jnp.exp(math.log(4.0) - 2.0794415 * jax.random.uniform(streams_of[4], (NL, NX, NY), jnp.float32) ** steps_of(streams_of[4], (NL, NX, NY), ((0, 2), (1, 4), (2, 4)), -0.2, 0.2)), 0.5, 4.0),
        "via_density": jnp.clip(jnp.exp(math.log(4.0) - 2.0794415 * jax.random.uniform(streams_of[5], (NX, NY), jnp.float32) ** steps_of(streams_of[5], (NX, NY), ((0, 4), (1, 4)), -0.2, 0.2)), 0.5, 4.0),
        "pad": jnp.clip(jnp.exp(math.log(0.5) - 2.3025851 * jax.random.uniform(streams_of[6], (NX, NY), jnp.float32) ** steps_of(streams_of[6], (NX, NY), ((0, 4), (1, 4)), -0.2, 0.2)), 0.05, 0.5),
        "start_drop": jnp.clip(1.0 * jax.random.uniform(streams_of[7], (NL, NX, NY), jnp.float32) ** steps_of(streams_of[7], (NL, NX, NY), ((0, 2), (1, 4), (2, 4)), -0.2, 0.2), 0.0, 1.0),
    }


def harmonic(values, beside):
    return 2.0 * values * beside / (values + beside)


def links(extended, via_column):
    middle = extended[1:-1, 1:-1, 1:-1]
    east_link = harmonic(middle, extended[1:-1, 2:, 1:-1])
    west_link = harmonic(middle, extended[1:-1, :-2, 1:-1])
    north_link = harmonic(middle, extended[1:-1, 1:-1, 2:])
    south_link = harmonic(middle, extended[1:-1, 1:-1, :-2])
    upper_link = via_column * harmonic(middle, extended[2:, 1:-1, 1:-1])
    lower_link = via_column * harmonic(middle, extended[:-2, 1:-1, 1:-1])
    return (east_link, west_link, north_link, south_link, upper_link, lower_link)


def diagonal_of(conduct):
    east_link, west_link, north_link, south_link, upper_link, lower_link = conduct
    return east_link + west_link + north_link + south_link + upper_link + lower_link


def operate(field, extended, conduct, diagonal):
    east_link, west_link, north_link, south_link, upper_link, lower_link = conduct
    result = diagonal * field - east_link * extended[1:-1, 2:, 1:-1] - west_link * extended[1:-1, :-2, 1:-1]
    result = result - north_link * extended[1:-1, 1:-1, 2:] - south_link * extended[1:-1, 1:-1, :-2]
    return result - upper_link * extended[2:, 1:-1, 1:-1] - lower_link * extended[:-2, 1:-1, 1:-1]


def reference(profiles, time_weight, slot_cell, inst_count, metal, via_density, pad, start_drop):
    slot_current = jnp.dot(profiles.reshape(-1, TIME), time_weight, preferred_element_type=jnp.float32)
    slot_current = slot_current.reshape(GROUPS, TILES_X, TILES_Y, INST_DEV)
    positions = jnp.arange(INST_DEV, dtype=jnp.int32)
    slot_current = jnp.where(positions[None, None, None, :] < inst_count[..., None], slot_current, 0.0)
    cells = slot_cell.reshape(GROUPS, TILES_X, TILES_Y, INST_DEV)
    row_base = (jnp.arange(TILES_X, dtype=jnp.int32) * CX)[None, :, None, None]
    col_base = (jnp.arange(TILES_Y, dtype=jnp.int32) * CY)[None, None, :, None]
    flat_index = ((cells // CY + row_base) * NY + cells % CY + col_base).reshape(-1).astype(jnp.int32)
    current = jax.ops.segment_sum(slot_current.reshape(-1), flat_index, num_segments=NX * NY).reshape(NX, NY)
    rhs = jnp.zeros_like(metal).at[0].set(current.astype(metal.dtype))
    conduct = links(jnp.pad(metal, 1), via_density[None])
    diagonal = diagonal_of(conduct).at[-1].add(pad)

    def apply(field):
        return operate(field, jnp.pad(field, 1), conduct, diagonal)

    solution = start_drop
    residual = rhs - apply(start_drop)
    scaled = residual / diagonal
    direction = scaled
    energy = jnp.sum(residual * scaled)
    for iteration in range(ITERS):
        image = apply(direction)
        step_size = energy / jnp.sum(direction * image)
        solution = solution + step_size * direction
        residual = residual - step_size * image
        if iteration + 1 < ITERS:
            scaled = residual / diagonal
            energy_next = jnp.sum(residual * scaled)
            direction = scaled + (energy_next / energy) * direction
            energy = energy_next
    return solution, residual
```

```python
import functools

import jax
import jax.numpy as jnp
from jax import lax
from jax.experimental import pallas as pl
from jax.experimental.pallas import tpu as pltpu
from jax.sharding import PartitionSpec as P

ITERS = 3
PAD = 8
LANES = 128
WIDE = 256
MESH = pl.DeviceIdType.MESH


def harmonic(values, beside):
    return 2.0 * values * beside / (values + beside)


def cg_coefficients(moments):
    def form(left, right):
        total = None
        for a, x in enumerate(left):
            for b, y in enumerate(right):
                term = x * y * moments[a + b]
                total = term if total is None else total + term
        return total

    one = jnp.ones_like(moments[0])
    scaled, direction = [one], [one]
    moved = [jnp.zeros_like(one)] * ITERS
    energy = form(scaled, scaled)
    for iteration in range(ITERS):
        image = [
            (direction[c] if c < len(direction) else 0.0) - (direction[c - 1] if c else 0.0)
            for c in range(len(direction) + 1)
        ]
        step = energy / form(direction, image)
        for c, value in enumerate(direction):
            moved[c] = moved[c] + step * value
        scaled = [
            (scaled[c] if c < len(scaled) else 0.0) - step * image[c] for c in range(len(image))
        ]
        if iteration + 1 < ITERS:
            energy_next = form(scaled, scaled)
            momentum = energy_next / energy
            direction = [
                scaled[c] + (momentum * direction[c] if c < len(direction) else 0.0)
                for c in range(len(scaled))
            ]
            energy = energy_next
    return moved, scaled


def kernel(
    sizes, slots, profiles, weight, cells, count, metal, via, pad, start, drop, residual,
    pbuf, psem, acc, cur_recv, dinv, diag, coef, field, rows_send, rows_recv, cols_pack, cols_send, cols_recv,
    plane_recv, col_halo, sums, gather, send_sem, recv_sem, gsend, grecv,
):
    ngx, ngy, nlayer = sizes
    total = ngx * ngy * nlayer
    nl, nr, nc = metal.shape
    gx, gy, layer = lax.axis_index("gx"), lax.axis_index("gy"), lax.axis_index("layer")
    me = (gx * ngy + gy) * nlayer + layer
    chunks = pbuf.shape[0]

    def coords(flat):
        return (flat // (ngy * nlayer), (flat // nlayer) % ngy, flat % nlayer)

    barrier = pltpu.get_barrier_semaphore()

    def greet(k, carry):
        peer = lax.rem(me + k, total)
        pl.semaphore_signal(barrier, inc=1, device_id=coords(peer), device_id_type=MESH)
        return carry

    lax.fori_loop(1, total, greet, 0)

    for i in range(chunks):
        pltpu.make_async_copy(profiles.at[i], pbuf.at[i], psem.at[i]).start()

    lane = lax.broadcasted_iota(jnp.int32, (nr, LANES), 1)

    def pack_columns(first_of, last_of, count_of):
        packed = jnp.zeros((nr, LANES), jnp.float32)
        for l in range(count_of):
            packed = jnp.where(lane == l, last_of(l), packed)
            packed = jnp.where(lane == 8 + l, first_of(l), packed)
        return packed

    def exchange(e):
        own = layer
        def copy(src, dst, k, device):
            return pltpu.make_async_remote_copy(
                src_ref=src, dst_ref=dst, send_sem=send_sem.at[e, k], recv_sem=recv_sem.at[e, k],
                device_id=device, device_id_type=MESH,
            )
        plane = (1 - own) * (nl - 1)
        if e == 0:
            planes = [(metal.at[plane], plane_recv.at[0]), (start.at[plane], plane_recv.at[1])]
        else:
            planes = [(field.at[e - 1, plane, pl.ds(PAD, nr)], plane_recv.at[e + 1])]
        partner = (gx, gy, 1 - layer)
        return {
            "down": (gx < ngx - 1, copy(rows_send.at[e, 0], rows_recv.at[e, 0], 0, (lax.min(gx + 1, ngx - 1), gy, layer))),
            "up": (gx > 0, copy(rows_send.at[e, 1], rows_recv.at[e, 1], 1, (lax.max(gx - 1, 0), gy, layer))),
            "right": (gy < ngy - 1, copy(cols_send.at[e, pl.ds(0, 8)], cols_recv.at[e, 0], 2, (gx, lax.min(gy + 1, ngy - 1), layer))),
            "left": (gy > 0, copy(cols_send.at[e, pl.ds(8, 8)], cols_recv.at[e, 1], 3, (gx, lax.max(gy - 1, 0), layer))),
            "planes": [copy(s, d, 4 + i, partner) for i, (s, d) in enumerate(planes)],
        }

    def begin(e):
        ops = exchange(e)
        for op in ops["planes"]:
            op.start()
        for name in ("down", "up", "right", "left"):
            there, op = ops[name]

            @pl.when(there)
            def _():
                op.start()

    def finish(e):
        ops = exchange(e)
        arrives = {"down": gx > 0, "up": gx < ngx - 1, "right": gy > 0, "left": gy < ngy - 1}
        places = {
            "down": rows_recv.at[e, 0], "up": rows_recv.at[e, 1],
            "right": cols_recv.at[e, 0], "left": cols_recv.at[e, 1],
        }
        for name in ("down", "up", "right", "left"):
            there, op = ops[name]

            @pl.when(there)
            def _():
                op.wait_send()

            @pl.when(arrives[name])
            def _():
                op.wait_recv()

            @pl.when(jnp.logical_not(arrives[name]))
            def _():
                places[name][...] = jnp.zeros(places[name].shape, jnp.float32)
        for op in ops["planes"]:
            op.wait()
        halo = jnp.concatenate(
            [cols_recv[e, 0], cols_recv[e, 1], jnp.zeros((LANES - 16, nr), jnp.float32)], axis=0
        )
        col_halo[...] = jnp.transpose(halo)

    both = (metal, start)
    for l in range(2 * nl):
        ref = both[l // nl]
        rows_send[0, 0, pl.ds(l, 1), :] = ref[l % nl, pl.ds(nr - 1, 1), :]
        rows_send[0, 1, pl.ds(l, 1), :] = ref[l % nl, pl.ds(0, 1), :]
    packed = pack_columns(
        lambda l: both[l // nl][l % nl, :, pl.ds(0, LANES)][:, 0:1],
        lambda l: both[l // nl][l % nl, :, pl.ds(nc - LANES, LANES)][:, LANES - 1 :],
        2 * nl,
    )
    cols_send[0] = jnp.transpose(packed)[0:16]
    pl.semaphore_wait(barrier, total - 1)
    begin(0)

    halves = nc // WIDE
    high = nr * halves
    acc[...] = jnp.zeros_like(acc)
    ids = lax.broadcasted_iota(jnp.int32, (max(high, WIDE), LANES), 0).astype(jnp.float32).astype(jnp.bfloat16)
    live = count[0, 0, 0]
    wide_weight = jnp.broadcast_to(weight[...], (16, weight.shape[1]))
    nt = (((1,), (1,)), ((), ()))
    for i in range(chunks):
        pltpu.make_async_copy(profiles.at[i], pbuf.at[i], psem.at[i]).wait()

        amounts = lax.dot_general(wide_weight, pbuf[i], nt, preferred_element_type=jnp.float32)[0:1]
        position = i * slots + lax.broadcasted_iota(jnp.int32, (1, slots), 1)
        amounts = jnp.where(position < live, amounts, 0.0).astype(jnp.bfloat16)
        cell = cells[i]
        column = lax.rem(cell, nc)
        tall = lax.div(column, WIDE) * nr + lax.div(cell, nc)
        tall = tall.astype(jnp.float32).astype(jnp.bfloat16)
        short = lax.rem(column, WIDE).astype(jnp.float32).astype(jnp.bfloat16)
        left, right = [], []
        zero, one = jnp.zeros((), jnp.bfloat16), jnp.ones((), jnp.bfloat16)
        for g in range(slots // LANES):
            part = slice(g * LANES, (g + 1) * LANES)
            left.append(jnp.where(ids[:high] == tall[:, part], jnp.broadcast_to(amounts[:, part], (high, LANES)), zero))
            right.append(jnp.where(ids[:WIDE] == short[:, part], one, zero))
        acc[...] += lax.dot_general(
            jnp.concatenate(left, axis=1), jnp.concatenate(right, axis=1), nt,
            preferred_element_type=jnp.float32,
        )

    def current_copy():
        return pltpu.make_async_remote_copy(
            src_ref=acc, dst_ref=cur_recv, send_sem=send_sem.at[0, 6], recv_sem=recv_sem.at[0, 6],
            device_id=(gx, gy, 1 - layer), device_id_type=MESH,
        )

    current_copy().start()

    finish(0)
    lane_all = lax.broadcasted_iota(jnp.int32, (nr, nc), 1)
    row_all = lax.broadcasted_iota(jnp.int32, (nr, nc), 0)

    def beside(value, above, below, before, after):
        north_of = jnp.where(lane_all == nc - 1, after, pltpu.roll(value, nc - 1, 1))
        south_of = jnp.where(lane_all == 0, before, pltpu.roll(value, 1, 1))
        east_of = jnp.where(row_all == nr - 1, below, pltpu.roll(value, nr - 1, 0))
        west_of = jnp.where(row_all == 0, above, pltpu.roll(value, 1, 0))
        return east_of, west_of, north_of, south_of

    first = layer == 0
    for l in range(nl):
        value = metal[l]
        around = beside(
            value, rows_recv[0, 0, pl.ds(l, 1), :], rows_recv[0, 1, pl.ds(l, 1), :],
            col_halo[:, l : l + 1], col_halo[:, 8 + l : 9 + l],
        )
        links = [harmonic(value, other) for other in around]
        upper = metal[l + 1] if l + 1 < nl else jnp.where(first, plane_recv[0], 0.0)
        lower = metal[l - 1] if l else jnp.where(first, 0.0, plane_recv[0])
        links += [via[...] * harmonic(value, other) for other in (upper, lower)]
        whole = links[0] + links[1] + links[2] + links[3] + links[4] + links[5]
        if l + 1 == nl:
            whole = whole + jnp.where(first, 0.0, pad[...])
        diag[l] = whole
        inverse = 1.0 / whole
        dinv[l] = inverse
        for k in range(6):
            coef[k, l] = links[k] * inverse

    def smooth(l, value, above, below, before, after, upper, lower):
        around = beside(value, above, below, before, after)
        out = coef[0, l] * around[0] + coef[1, l] * around[1] + coef[2, l] * around[2] + coef[3, l] * around[3]
        return out + coef[4, l] * upper + coef[5, l] * lower

    def send_field(e):
        f = e - 1
        for l in range(nl):
            rows_send[e, 0, pl.ds(l, 1), :] = field[f, l, pl.ds(PAD + nr - 1, 1), :]
            rows_send[e, 1, pl.ds(l, 1), :] = field[f, l, pl.ds(PAD, 1), :]
        packed = pack_columns(
            lambda l: field[f, l, pl.ds(PAD, nr), pl.ds(0, LANES)][:, 0:1],
            lambda l: field[f, l, pl.ds(PAD, nr), pl.ds(nc - LANES, LANES)][:, LANES - 1 :],
            nl,
        )
        cols_send[e] = jnp.transpose(packed)[0:16]
        begin(e)

    mapped = []
    for l in range(nl):
        value = start[l]
        moved = smooth(
            l, value, rows_recv[0, 0, pl.ds(nl + l, 1), :], rows_recv[0, 1, pl.ds(nl + l, 1), :],
            col_halo[:, nl + l : nl + l + 1], col_halo[:, 8 + nl + l : 9 + nl + l],
            start[l + 1] if l + 1 < nl else plane_recv[1], start[l - 1] if l else plane_recv[1],
        )
        field[0, l, pl.ds(PAD, nr), :] = moved - value
    current_copy().wait()
    gathered = acc[...] + cur_recv[...]
    current = jnp.concatenate([gathered[h * nr : (h + 1) * nr] for h in range(halves)], axis=1)
    field[0, 0, pl.ds(PAD, nr), :] += jnp.where(first, dinv[0] * current, 0.0)

    tiles = []
    for e in range(1, ITERS + 1):
        f = e - 1
        send_field(e)
        finish(e)
        even, odd = None, None
        for l in range(nl):
            value = field[f, l, pl.ds(PAD, nr), :]
            upper = field[f, l + 1, pl.ds(PAD, nr), :] if l + 1 < nl else plane_recv[e + 1]
            lower = field[f, l - 1, pl.ds(PAD, nr), :] if l else plane_recv[e + 1]
            moved = smooth(
                l, value, rows_recv[e, 0, pl.ds(l, 1), :], rows_recv[e, 1, pl.ds(l, 1), :],
                col_halo[:, l : l + 1], col_halo[:, 8 + l : 9 + l], upper, lower,
            )
            field[e, l, pl.ds(PAD, nr), :] = moved
            heavy = diag[l] * value
            a = jnp.sum(heavy * value, axis=0, keepdims=True)
            b = jnp.sum(heavy * moved, axis=0, keepdims=True)
            even = a if even is None else even + a
            odd = b if odd is None else odd + b
        tiles += [even, odd]

    row = lax.broadcasted_iota(jnp.int32, (1, LANES), 1)
    packed = jnp.zeros((1, LANES), jnp.float32)
    for j, tile in enumerate(tiles):
        packed = jnp.where(row == j, jnp.sum(tile, axis=1, keepdims=True), packed)
    sums[...] = packed
    gather[me] = packed

    def tell(k, carry):
        peer = lax.rem(me + k, total)
        pltpu.make_async_remote_copy(
            src_ref=sums, dst_ref=gather.at[me], send_sem=gsend, recv_sem=grecv,
            device_id=coords(peer), device_id_type=MESH,
        ).start()
        return carry

    lax.fori_loop(1, total, tell, 0)
    most = gather.at[pl.ds(0, total - 1)]
    pltpu.make_async_copy(most, most, grecv).wait()
    pltpu.make_async_copy(most, most, gsend).wait()
    summed = jnp.sum(gather[...], axis=0)
    moments = [jnp.sum(jnp.where(row == j, summed, 0.0), axis=1, keepdims=True) for j in range(2 * ITERS)]
    moved, scaled = cg_coefficients(moments)
    for l in range(nl):
        parts = [field[c, l, pl.ds(PAD, nr), :] for c in range(ITERS + 1)]
        out = start[l]
        for c in range(ITERS):
            out = out + moved[c] * parts[c]
        drop[l] = out
        rest = scaled[0] * parts[0]
        for c in range(1, ITERS + 1):
            rest = rest + scaled[c] * parts[c]
        residual[l] = diag[l] * rest


def per_device(sizes, profiles, time_weight, slot_cell, inst_count, metal, via_density, pad, start_drop):
    nl, nr, nc = metal.shape
    inst, times = profiles.shape[-2:]
    slots = min(1024, inst)
    chunks = inst // slots
    total = sizes[0] * sizes[1] * sizes[2]
    vmem = pl.BlockSpec(memory_space=pltpu.VMEM)
    high = nr * (nc // WIDE)
    f32 = jnp.float32
    out = jax.ShapeDtypeStruct((nl, nr, nc), f32)
    exchanges = ITERS + 1
    return pl.pallas_call(
        functools.partial(kernel, sizes, slots),
        out_shape=(out, out),
        in_specs=[
            pl.BlockSpec(memory_space=pl.ANY), vmem, vmem, pl.BlockSpec(memory_space=pltpu.SMEM),
            vmem, vmem, vmem, vmem,
        ],
        out_specs=(vmem, vmem),
        scratch_shapes=[
            pltpu.VMEM((chunks, slots, times), jnp.bfloat16),
            pltpu.SemaphoreType.DMA((chunks,)),
            pltpu.VMEM((high, WIDE), f32),
            pltpu.VMEM((high, WIDE), f32),
            pltpu.VMEM((nl, nr, nc), f32),
            pltpu.VMEM((nl, nr, nc), f32),
            pltpu.VMEM((6, nl, nr, nc), f32),
            pltpu.VMEM((exchanges, nl, nr + 2 * PAD, nc), f32),
            pltpu.VMEM((exchanges, 2, 8, nc), f32),
            pltpu.VMEM((exchanges, 2, 8, nc), f32),
            pltpu.VMEM((nr, LANES), f32),
            pltpu.VMEM((exchanges, 16, nr), f32),
            pltpu.VMEM((exchanges, 2, 8, nr), f32),
            pltpu.VMEM((exchanges + 1, nr, nc), f32),
            pltpu.VMEM((nr, LANES), f32),
            pltpu.VMEM((1, LANES), f32),
            pltpu.VMEM((total, 1, LANES), f32),
            pltpu.SemaphoreType.DMA((exchanges, 7)),
            pltpu.SemaphoreType.DMA((exchanges, 7)),
            pltpu.SemaphoreType.DMA,
            pltpu.SemaphoreType.DMA,
        ],
        compiler_params=pltpu.CompilerParams(
            collective_id=0, has_side_effects=True, vmem_limit_bytes=56 * 1024 * 1024
        ),
    )(
        profiles.reshape(chunks, slots, times), time_weight.reshape(1, times),
        slot_cell.reshape(chunks, 1, slots), inst_count, metal, via_density, pad, start_drop,
    )


def solution(mesh):
    sizes = tuple(mesh.shape[axis] for axis in ("gx", "gy", "layer"))
    in_specs = (
        P("layer", "gx", "gy", None),
        P(),
        P("layer", "gx", "gy"),
        P("layer", "gx", "gy"),
        P("layer", "gx", "gy"),
        P("gx", "gy"),
        P("gx", "gy"),
        P("layer", "gx", "gy"),
    )
    out_specs = (P("layer", "gx", "gy"), P("layer", "gx", "gy"))
    return jax.shard_map(
        functools.partial(per_device, sizes), mesh=mesh, in_specs=in_specs, out_specs=out_specs, check_vma=False
    )
```

```python
import functools

import jax
import jax.numpy as jnp
from jax import lax
from jax.experimental import pallas as pl
from jax.experimental.pallas import tpu as pltpu
from jax.sharding import PartitionSpec as P

ITERS = 3
PAD = 8
LANES = 128
WIDE = 256
MESH = pl.DeviceIdType.MESH


def harmonic(values, beside):
    return 2.0 * values * beside / (values + beside)


def div_by(values, size):
    if size & (size - 1) == 0:
        return lax.shift_right_logical(values, jnp.full_like(values, size.bit_length() - 1))
    return lax.div(values, size)


def rem_by(values, size):
    return values & (size - 1) if size & (size - 1) == 0 else lax.rem(values, size)


def cg_coefficients(moments):
    def form(left, right):
        total = None
        for a, x in enumerate(left):
            for b, y in enumerate(right):
                term = x * y * moments[a + b]
                total = term if total is None else total + term
        return total

    one = jnp.ones_like(moments[0])
    scaled, direction = [one], [one]
    moved = [jnp.zeros_like(one)] * ITERS
    energy = form(scaled, scaled)
    for iteration in range(ITERS):
        image = [
            (direction[c] if c < len(direction) else 0.0) - (direction[c - 1] if c else 0.0)
            for c in range(len(direction) + 1)
        ]
        step = energy / form(direction, image)
        for c, value in enumerate(direction):
            moved[c] = moved[c] + step * value
        scaled = [
            (scaled[c] if c < len(scaled) else 0.0) - step * image[c] for c in range(len(image))
        ]
        if iteration + 1 < ITERS:
            energy_next = form(scaled, scaled)
            momentum = energy_next / energy
            direction = [
                scaled[c] + (momentum * direction[c] if c < len(direction) else 0.0)
                for c in range(len(scaled))
            ]
            energy = energy_next
    return moved, scaled


def kernel(
    sizes, slots, profiles, weight, cells, count, metal, via, pad, start, drop, residual,
    pbuf, psem, acc, cur_recv, dinv, diag, coef, field, rows_send, rows_recv, cols_pack, cols_send, cols_recv,
    plane_recv, col_halo, sums, gather, send_sem, recv_sem, gsend, grecv,
):
    ngx, ngy, nlayer = sizes
    total = ngx * ngy * nlayer
    nl, nr, nc = metal.shape
    gx, gy, layer = lax.axis_index("gx"), lax.axis_index("gy"), lax.axis_index("layer")
    me = (gx * ngy + gy) * nlayer + layer
    chunks = pbuf.shape[0]

    def coords(flat):
        return (flat // (ngy * nlayer), (flat // nlayer) % ngy, flat % nlayer)

    barrier = pltpu.get_barrier_semaphore()

    def greet(k, carry):
        peer = lax.rem(me + k, total)
        pl.semaphore_signal(barrier, inc=1, device_id=coords(peer), device_id_type=MESH)
        return carry

    lax.fori_loop(1, total, greet, 0)

    for i in range(chunks):
        pltpu.make_async_copy(profiles.at[i], pbuf.at[i], psem.at[i]).start()

    lane = lax.broadcasted_iota(jnp.int32, (nr, LANES), 1)

    def pack_columns(first_of, last_of, count_of):
        packed = jnp.zeros((nr, LANES), jnp.float32)
        for l in range(count_of):
            packed = jnp.where(lane == l, last_of(l), packed)
            packed = jnp.where(lane == 8 + l, first_of(l), packed)
        return packed

    def exchange(e):
        own = layer
        def copy(src, dst, k, device):
            return pltpu.make_async_remote_copy(
                src_ref=src, dst_ref=dst, send_sem=send_sem.at[e, k], recv_sem=recv_sem.at[e, k],
                device_id=device, device_id_type=MESH,
            )
        plane = (1 - own) * (nl - 1)
        if e == 0:
            planes = [(metal.at[plane], plane_recv.at[0]), (start.at[plane], plane_recv.at[1])]
        else:
            planes = [(field.at[e - 1, plane, pl.ds(PAD, nr)], plane_recv.at[e + 1])]
        partner = (gx, gy, 1 - layer)
        return {
            "down": (gx < ngx - 1, copy(rows_send.at[e, 0], rows_recv.at[e, 0], 0, (lax.min(gx + 1, ngx - 1), gy, layer))),
            "up": (gx > 0, copy(rows_send.at[e, 1], rows_recv.at[e, 1], 1, (lax.max(gx - 1, 0), gy, layer))),
            "right": (gy < ngy - 1, copy(cols_send.at[e, pl.ds(0, 8)], cols_recv.at[e, 0], 2, (gx, lax.min(gy + 1, ngy - 1), layer))),
            "left": (gy > 0, copy(cols_send.at[e, pl.ds(8, 8)], cols_recv.at[e, 1], 3, (gx, lax.max(gy - 1, 0), layer))),
            "planes": [copy(s, d, 4 + i, partner) for i, (s, d) in enumerate(planes)],
        }

    def begin(e):
        ops = exchange(e)
        for op in ops["planes"]:
            op.start()
        for name in ("down", "up", "right", "left"):
            there, op = ops[name]

            @pl.when(there)
            def _():
                op.start()

    def finish(e):
        ops = exchange(e)
        arrives = {"down": gx > 0, "up": gx < ngx - 1, "right": gy > 0, "left": gy < ngy - 1}
        places = {
            "down": rows_recv.at[e, 0], "up": rows_recv.at[e, 1],
            "right": cols_recv.at[e, 0], "left": cols_recv.at[e, 1],
        }
        for name in ("down", "up", "right", "left"):
            there, op = ops[name]

            @pl.when(there)
            def _():
                op.wait_send()

            @pl.when(arrives[name])
            def _():
                op.wait_recv()

            @pl.when(jnp.logical_not(arrives[name]))
            def _():
                places[name][...] = jnp.zeros(places[name].shape, jnp.float32)
        for op in ops["planes"]:
            op.wait()
        halo = jnp.concatenate(
            [cols_recv[e, 0], cols_recv[e, 1], jnp.zeros((LANES - 16, nr), jnp.float32)], axis=0
        )
        col_halo[...] = jnp.transpose(halo)

    both = (metal, start)
    for l in range(2 * nl):
        ref = both[l // nl]
        rows_send[0, 0, pl.ds(l, 1), :] = ref[l % nl, pl.ds(nr - 1, 1), :]
        rows_send[0, 1, pl.ds(l, 1), :] = ref[l % nl, pl.ds(0, 1), :]
    packed = pack_columns(
        lambda l: both[l // nl][l % nl, :, pl.ds(0, LANES)][:, 0:1],
        lambda l: both[l // nl][l % nl, :, pl.ds(nc - LANES, LANES)][:, LANES - 1 :],
        2 * nl,
    )
    cols_send[0] = jnp.transpose(packed)[0:16]
    pl.semaphore_wait(barrier, total - 1)
    begin(0)

    halves = nc // WIDE
    high = nr * halves
    acc[...] = jnp.zeros_like(acc)
    ids = lax.broadcasted_iota(jnp.int32, (max(high, WIDE), LANES), 0).astype(jnp.float32).astype(jnp.bfloat16)
    live = count[0]
    wide_weight = jnp.broadcast_to(weight[...], (16, weight.shape[1]))
    nt = (((1,), (1,)), ((), ()))
    for i in range(chunks):
        pltpu.make_async_copy(profiles.at[i], pbuf.at[i], psem.at[i]).wait()

        amounts = lax.dot_general(wide_weight, pbuf[i], nt, preferred_element_type=jnp.float32)[0:1]
        position = i * slots + lax.broadcasted_iota(jnp.int32, (1, slots), 1)
        amounts = jnp.where(position < live, amounts, 0.0).astype(jnp.bfloat16)
        cell = cells[i]
        column = rem_by(cell, nc)
        tall = div_by(column, WIDE) * nr + div_by(cell, nc)
        tall = tall.astype(jnp.float32).astype(jnp.bfloat16)
        short = rem_by(column, WIDE).astype(jnp.float32).astype(jnp.bfloat16)
        left, right = [], []
        zero, one = jnp.zeros((), jnp.bfloat16), jnp.ones((), jnp.bfloat16)
        for g in range(slots // LANES):
            part = slice(g * LANES, (g + 1) * LANES)
            left.append(jnp.where(ids[:high] == tall[:, part], jnp.broadcast_to(amounts[:, part], (high, LANES)), zero))
            right.append(jnp.where(ids[:WIDE] == short[:, part], one, zero))
        acc[...] += lax.dot_general(
            jnp.concatenate(left, axis=1), jnp.concatenate(right, axis=1), nt,
            preferred_element_type=jnp.float32,
        )

    def current_copy():
        return pltpu.make_async_remote_copy(
            src_ref=acc, dst_ref=cur_recv, send_sem=send_sem.at[0, 6], recv_sem=recv_sem.at[0, 6],
            device_id=(gx, gy, 1 - layer), device_id_type=MESH,
        )

    current_copy().start()

    finish(0)
    lane_all = lax.broadcasted_iota(jnp.int32, (nr, nc), 1)
    row_all = lax.broadcasted_iota(jnp.int32, (nr, nc), 0)

    def beside(value, above, below, before, after):
        north_of = jnp.where(lane_all == nc - 1, after, pltpu.roll(value, nc - 1, 1))
        south_of = jnp.where(lane_all == 0, before, pltpu.roll(value, 1, 1))
        east_of = jnp.where(row_all == nr - 1, below, pltpu.roll(value, nr - 1, 0))
        west_of = jnp.where(row_all == 0, above, pltpu.roll(value, 1, 0))
        return east_of, west_of, north_of, south_of

    first = layer == 0
    for l in range(nl):
        value = metal[l]
        around = beside(
            value, rows_recv[0, 0, pl.ds(l, 1), :], rows_recv[0, 1, pl.ds(l, 1), :],
            col_halo[:, l : l + 1], col_halo[:, 8 + l : 9 + l],
        )
        links = [harmonic(value, other) for other in around]
        upper = metal[l + 1] if l + 1 < nl else jnp.where(first, plane_recv[0], 0.0)
        lower = metal[l - 1] if l else jnp.where(first, 0.0, plane_recv[0])
        links += [via[...] * harmonic(value, other) for other in (upper, lower)]
        whole = links[0] + links[1] + links[2] + links[3] + links[4] + links[5]
        if l + 1 == nl:
            whole = whole + jnp.where(first, 0.0, pad[...])
        diag[l] = whole
        inverse = 1.0 / whole
        dinv[l] = inverse
        for k in range(6):
            coef[k, l] = links[k] * inverse

    def inside(l, value, upper, lower):
        around = beside(value, 0.0, 0.0, 0.0, 0.0)
        out = coef[0, l] * around[0] + coef[1, l] * around[1] + coef[2, l] * around[2] + coef[3, l] * around[3]
        if upper is not None:
            out = out + coef[4, l] * upper
        if lower is not None:
            out = out + coef[5, l] * lower
        return out

    edge = (1 - layer) * (nl - 1)
    lane_west = lane == 0
    lane_east = lane == LANES - 1

    def across(f, shift, e, plane, weigh):
        odd = jnp.zeros((1, LANES), jnp.float32)

        def narrow(tile):
            wide = jnp.sum(tile, axis=0, keepdims=True)
            return functools.reduce(jnp.add, [wide[:, k : k + LANES] for k in range(0, wide.shape[1], LANES)])

        def add(l, rows, columns, first_row, term):
            odd = None
            field[f, l, pl.ds(PAD + first_row, rows), columns] += term
            if weigh is not None:
                heavy = diag[l, pl.ds(first_row, rows), columns] * field[weigh, l, pl.ds(PAD + first_row, rows), columns]
                odd = narrow(heavy * term)
            return odd

        parts = []
        everywhere = pl.ds(0, nc)
        for l in range(nl):
            parts.append(add(l, 1, everywhere, 0, coef[1, l, pl.ds(0, 1), :] * rows_recv[e, 0, pl.ds(shift + l, 1), :]))
            parts.append(add(l, 1, everywhere, nr - 1, coef[0, l, pl.ds(nr - 1, 1), :] * rows_recv[e, 1, pl.ds(shift + l, 1), :]))
            k = shift + l
            west, east = pl.ds(0, LANES), pl.ds(nc - LANES, LANES)
            parts.append(add(l, nr, west, 0, jnp.where(lane_west, coef[3, l, :, west] * col_halo[:, k : k + 1], 0.0)))
            parts.append(add(l, nr, east, 0, jnp.where(lane_east, coef[2, l, :, east] * col_halo[:, 8 + k : 9 + k], 0.0)))
        parts.append(add(edge, nr, everywhere, 0, coef[4 + layer, edge] * plane_recv[plane]))
        if weigh is not None:
            odd = functools.reduce(jnp.add, parts)
        return odd

    def send_field(e):
        f = e - 1
        for l in range(nl):
            rows_send[e, 0, pl.ds(l, 1), :] = field[f, l, pl.ds(PAD + nr - 1, 1), :]
            rows_send[e, 1, pl.ds(l, 1), :] = field[f, l, pl.ds(PAD, 1), :]
        packed = pack_columns(
            lambda l: field[f, l, pl.ds(PAD, nr), pl.ds(0, LANES)][:, 0:1],
            lambda l: field[f, l, pl.ds(PAD, nr), pl.ds(nc - LANES, LANES)][:, LANES - 1 :],
            nl,
        )
        cols_send[e] = jnp.transpose(packed)[0:16]
        begin(e)

    for l in range(nl):
        value = start[l]
        moved = inside(l, value, start[l + 1] if l + 1 < nl else None, start[l - 1] if l else None)
        field[0, l, pl.ds(PAD, nr), :] = moved - value
    across(0, nl, 0, 1, None)
    current_copy().wait()
    gathered = acc[...] + cur_recv[...]
    current = jnp.concatenate([gathered[h * nr : (h + 1) * nr] for h in range(halves)], axis=1)
    field[0, 0, pl.ds(PAD, nr), :] += jnp.where(first, dinv[0] * current, 0.0)

    tiles = []
    for e in range(1, ITERS + 1):
        f = e - 1
        send_field(e)
        even, odd = None, None
        for l in range(nl):
            value = field[f, l, pl.ds(PAD, nr), :]
            upper = field[f, l + 1, pl.ds(PAD, nr), :] if l + 1 < nl else None
            lower = field[f, l - 1, pl.ds(PAD, nr), :] if l else None
            moved = inside(l, value, upper, lower)
            field[e, l, pl.ds(PAD, nr), :] = moved
            heavy = diag[l] * value
            a = jnp.sum(heavy * value, axis=0, keepdims=True)
            b = jnp.sum(heavy * moved, axis=0, keepdims=True)
            even = a if even is None else even + a
            odd = b if odd is None else odd + b
        finish(e)
        more = across(e, 0, e, e + 1, f)
        tiles += [even, jnp.concatenate([odd[:, :LANES] + more, odd[:, LANES:]], axis=1)]

    row = lax.broadcasted_iota(jnp.int32, (1, LANES), 1)
    packed = jnp.zeros((1, LANES), jnp.float32)
    for j, tile in enumerate(tiles):
        packed = jnp.where(row == j, jnp.sum(tile, axis=1, keepdims=True), packed)
    sums[...] = packed
    gather[me] = packed

    def tell(k, carry):
        peer = lax.rem(me + k, total)
        pltpu.make_async_remote_copy(
            src_ref=sums, dst_ref=gather.at[me], send_sem=gsend, recv_sem=grecv,
            device_id=coords(peer), device_id_type=MESH,
        ).start()
        return carry

    lax.fori_loop(1, total, tell, 0)
    most = gather.at[pl.ds(0, total - 1)]
    pltpu.make_async_copy(most, most, grecv).wait()
    pltpu.make_async_copy(most, most, gsend).wait()
    summed = jnp.sum(gather[...], axis=0)
    moments = [jnp.sum(jnp.where(row == j, summed, 0.0), axis=1, keepdims=True) for j in range(2 * ITERS)]
    moved, scaled = cg_coefficients(moments)
    for l in range(nl):
        parts = [field[c, l, pl.ds(PAD, nr), :] for c in range(ITERS + 1)]
        out = start[l]
        for c in range(ITERS):
            out = out + moved[c] * parts[c]
        drop[l] = out
        rest = scaled[0] * parts[0]
        for c in range(1, ITERS + 1):
            rest = rest + scaled[c] * parts[c]
        residual[l] = diag[l] * rest


def per_device(sizes, profiles, time_weight, slot_cell, inst_count, metal, via_density, pad, start_drop):
    nl, nr, nc = metal.shape
    inst, times = profiles.shape[-2:]
    slots = min(1024, inst)
    chunks = inst // slots
    total = sizes[0] * sizes[1] * sizes[2]
    vmem = pl.BlockSpec(memory_space=pltpu.VMEM)
    high = nr * (nc // WIDE)
    f32 = jnp.float32
    out = jax.ShapeDtypeStruct((nl, nr, nc), f32)
    exchanges = ITERS + 1
    return pl.pallas_call(
        functools.partial(kernel, sizes, slots),
        out_shape=(out, out),
        in_specs=[
            pl.BlockSpec(memory_space=pl.ANY), vmem, vmem, vmem,
            vmem, vmem, vmem, vmem,
        ],
        out_specs=(vmem, vmem),
        scratch_shapes=[
            pltpu.VMEM((chunks, slots, times), jnp.bfloat16),
            pltpu.SemaphoreType.DMA((chunks,)),
            pltpu.VMEM((high, WIDE), f32),
            pltpu.VMEM((high, WIDE), f32),
            pltpu.VMEM((nl, nr, nc), f32),
            pltpu.VMEM((nl, nr, nc), f32),
            pltpu.VMEM((6, nl, nr, nc), f32),
            pltpu.VMEM((exchanges, nl, nr + 2 * PAD, nc), f32),
            pltpu.VMEM((exchanges, 2, 8, nc), f32),
            pltpu.VMEM((exchanges, 2, 8, nc), f32),
            pltpu.VMEM((nr, LANES), f32),
            pltpu.VMEM((exchanges, 16, nr), f32),
            pltpu.VMEM((exchanges, 2, 8, nr), f32),
            pltpu.VMEM((exchanges + 1, nr, nc), f32),
            pltpu.VMEM((nr, LANES), f32),
            pltpu.VMEM((1, LANES), f32),
            pltpu.VMEM((total, 1, LANES), f32),
            pltpu.SemaphoreType.DMA((exchanges, 7)),
            pltpu.SemaphoreType.DMA((exchanges, 7)),
            pltpu.SemaphoreType.DMA,
            pltpu.SemaphoreType.DMA,
        ],
        compiler_params=pltpu.CompilerParams(
            collective_id=0, has_side_effects=True, vmem_limit_bytes=56 * 1024 * 1024
        ),
    )(
        profiles.reshape(chunks, slots, times), time_weight.reshape(1, times),
        slot_cell.reshape(chunks, 1, slots), inst_count, metal, via_density, pad, start_drop,
    )


def solution(mesh):
    sizes = tuple(mesh.shape[axis] for axis in ("gx", "gy", "layer"))
    in_specs = (
        P("layer", "gx", "gy", None),
        P(),
        P("layer", "gx", "gy"),
        P("layer", "gx", "gy"),
        P("layer", "gx", "gy"),
        P("gx", "gy"),
        P("gx", "gy"),
        P("layer", "gx", "gy"),
    )
    out_specs = (P("layer", "gx", "gy"), P("layer", "gx", "gy"))
    return jax.shard_map(
        functools.partial(per_device, sizes), mesh=mesh, in_specs=in_specs, out_specs=out_specs, check_vma=False
    )
```
